512 devices in a mesh: blk: 64 (over z_hi, x, y), grp: 8 (over z_lo, core).
Axes of the slice: x: 4, y: 8, z: 8 (z_hi: 2, z_lo: 4; z = z_hi * 4 + z_lo), core: 2. Of those that a mesh axis runs over, the one named last changes fastest.
Arguments:
- orbitals: bfloat16 [512, 64, 4096], P(('blk', 'grp')), may hold values from -6 to 6
- offsets: int32 [512, 3], replicated, may hold values from 0 to 15
- pair_list: int32 [512, 3], replicated, may hold values 0 or 1
Outputs:
- exchange_action: float32 [512, 64, 4096], P(('blk', 'grp'))
The draws below stay inside these ranges and needn't reach their ends.
All inputs are finite; a program needn't handle non-finite values.
Results may differ from the reference program's by a relative error of at most 0.0015.
Values may be sent and summed in bfloat16 or wider, within the bound.
No kernel may reach another device: no remote copies, remote signals or barrier semaphores. Data moves between devices by JAX's collectives and lax.ppermute only.
A program may use at most 128 MiB of HBM per device.

```python
import jax
import jax.numpy as jnp
from jax import lax

B = 64
REACH = 3
ORBITALS = 512


def plant(values, rng, low, largest):
    index_at = [jax.random.randint(jax.random.fold_in(rng, axis), (), 0, length) for axis, length in enumerate(values.shape)]
    widest = values.shape.index(max(values.shape))
    beside = index_at[:widest] + [(index_at[widest] + 1) % values.shape[widest]] + index_at[widest + 1:]
    return values.at[tuple(index_at)].set(low).at[tuple(beside)].set(largest)


def block_levels(rng, shape, pieces, low, largest):
    loudness, own = 1.0, jax.random.fold_in(rng, 6)
    for axis_at, shards_of in pieces:
        steps = jnp.exp(jax.random.uniform(jax.random.fold_in(own, axis_at), (shards_of,), jnp.float32, low / len(pieces), largest / len(pieces)))
        loudness = loudness * jnp.repeat(steps, shape[axis_at] // shards_of).reshape([-1 if axis == axis_at else 1 for axis in range(len(shape))])
    return loudness


def gaussian(stream_key, shape, scale, limit, cuts=(), kind=jnp.bfloat16):
    drawn = scale * jax.random.normal(stream_key, shape, jnp.float32)
    if cuts:
        drawn = drawn * block_levels(stream_key, shape, cuts, -0.22, 0.18)
    return jnp.clip(drawn, -limit, limit).astype(kind)


def setup_inputs(seed: int = 0) -> dict:
    key_list = jax.random.split(jax.random.key(seed), 4)
    orbitals = gaussian(key_list[0], (ORBITALS, B, B * B), 1.0, 6.0, ((0, 512),))
    offsets = plant(jax.random.randint(key_list[1], (ORBITALS, 3), 0, B // 4), jax.random.fold_in(key_list[1], 1), 0, (B // 4) - 1).astype(jnp.int32)
    pair_list = plant((jax.random.randint(key_list[2], (ORBITALS, REACH), 0, 4) < 3).astype(jnp.int32), jax.random.fold_in(key_list[2], 1), 0, 1)
    return dict(orbitals=orbitals, offsets=offsets, pair_list=pair_list)


KAPPA_SQ = 0.5
HIGHEST = lax.Precision.HIGHEST

def sine_matrix(extent):
    levels = jnp.arange(extent, dtype=jnp.float32) + 1.0
    return jnp.sqrt(2.0 / (extent + 1.0)) * jnp.sin(jnp.pi * levels[:, None] * levels[None, :] / (extent + 1.0))

def screened_kernel(extent):
    levels = jnp.arange(extent, dtype=jnp.float32) + 1.0
    eigen = 2.0 - 2.0 * jnp.cos(jnp.pi * levels / (extent + 1.0))
    return 1.0 / (eigen[:, None, None] + eigen[None, :, None] + eigen[None, None, :] + KAPPA_SQ)

def sine_transform(volume, sines):
    volume = jnp.einsum('ma,abc->mbc', sines, volume, precision=HIGHEST)
    volume = jnp.einsum('mb,abc->amc', sines, volume, precision=HIGHEST)
    return jnp.einsum('mc,abc->abm', sines, volume, precision=HIGHEST)

def screened_solve(density, sines, kernel):
    return sine_transform(kernel * sine_transform(density, sines), sines)

def moved_slice(volume, starts):
    extent = volume.shape[0]
    margin = extent // 4
    padded = jnp.pad(volume, margin)
    begin = tuple(((margin + starts[i]).astype(jnp.int32) for i in range(3)))
    return lax.dynamic_slice(padded, begin, (extent, extent, extent))

def into_box(volume, offset_gap):
    return moved_slice(volume, -offset_gap)

def back_to_box(volume, offset_gap):
    return moved_slice(volume, offset_gap)

def reference(orbitals, offsets, pair_list):
    total = orbitals.shape[0]
    volumes = orbitals.reshape(total, B, B, B).astype(jnp.float32)
    sines = sine_matrix(B)
    kernel = screened_kernel(B)

    def self_action(volume):
        return -screened_solve(volume * volume, sines, kernel) * volume
    action = lax.map(self_action, volumes)
    for distance in range(1, REACH + 1):
        below = jnp.roll(volumes, distance, axis=0)
        below_offsets = jnp.roll(offsets, distance, axis=0)
        weights = pair_list[:, distance - 1].astype(jnp.float32)

        def pair_action(item):
            resident, visitor, offset_gap, weight = item
            shifted = into_box(visitor, offset_gap)
            potential = screened_solve(resident * shifted, sines, kernel) * weight
            return (-potential * shifted, -back_to_box(potential * resident, offset_gap))
        kept, returned = lax.map(pair_action, (volumes, below, (below_offsets - offsets).astype(jnp.int32), weights))
        action = action + kept + jnp.roll(returned, -distance, axis=0)
    return action.reshape(total, B, B * B)
```

```python
import jax
import jax.numpy as jnp
import numpy as np
from jax import lax
from jax.experimental import pallas as pl
from jax.experimental.pallas import tpu as pltpu
from jax.sharding import PartitionSpec as P

B = 64
PITCH = 65
AXES = ("blk", "grp")


def constants():
    level = np.arange(1, B + 1, dtype=np.float64)
    sines = np.sqrt(2.0 / (B + 1)) * np.sin(np.pi * level[:, None] * level[None, :] / (B + 1))
    eigen = 2.0 - 2.0 * np.cos(np.pi * level / (B + 1))
    pair = eigen[:, None] + np.tile(eigen, 2)[None, :] + 0.5
    return [np.asarray(t, np.float32) for t in (np.pad(sines, ((0, 0), (32, 32))), pair, eigen)]


SEXT, LEV, LA = constants()
bf16, f32 = jnp.bfloat16, jnp.float32


def split(x):
    hi = x.astype(bf16)
    lo = (x - hi.astype(f32)).astype(bf16)
    return hi, lo


def dot(a, b):
    return jnp.dot(a, b, preferred_element_type=f32)


def iota(shape, dim):
    return lax.broadcasted_iota(jnp.int32, shape, dim)


def shifted_pair(sext, g0, g1):
    lane = iota((B, 128), 1)
    r0 = pltpu.roll(sext, (96 - g0) % 128, 1)
    r1 = pltpu.roll(sext, (160 - g1) % 128, 1)
    return jnp.concatenate([jnp.where(lane < B, r0, 0.0), jnp.where(lane >= B, r1, 0.0)], 0)


def lhs_quad(wide):
    lane = iota((128, 128), 1)
    both = wide + pltpu.roll(wide, 64, 1)
    hi, lo = split(both)
    return jnp.concatenate([hi, lo], 1)


def row_quad(wide):
    hi, lo = split(wide)
    top = jnp.concatenate([hi, lo], 1)
    bottom = jnp.concatenate([hi, jnp.zeros_like(lo)], 1)
    return jnp.concatenate([top, bottom], 0)


def rows_through(x, w):
    hi, lo = split(x)
    z = dot(jnp.concatenate([hi, lo], 1), w)
    return z[:, :128] + z[:, 128:]


def cols_through(lhs, x):
    hi, lo = split(x)
    z = dot(lhs, jnp.concatenate([hi, lo, hi, lo], 0))
    lane = iota((B, x.shape[1]), 1)
    return jnp.where(lane % 128 < B, z[:B], z[B:])


def neighbour(tab, nbr):
    count = lax.axis_size(AXES)
    here = lax.axis_index(AXES)
    if not nbr:
        return [0, 0, 0], 0, f32(1.0 if nbr == 0 else 0.0)
    step = jnp.where(here % 2 == 0, nbr, -nbr)
    there = lax.rem(here + step + count, count)
    gaps = [tab[d, here] - tab[d, there] for d in range(3)]
    up = step > 0
    weight = tab[2 + abs(nbr), jnp.where(up, there, here)].astype(f32)
    return gaps, jnp.where(up, 1, 0), weight


def pair_kernel(TB, TA, first, nbrs, tab, x_ref, n0_ref, n1_ref, acc_ref, sext_ref, lev_ref, la_ref, out_ref,
                xp0, xp1, y_ref, z_ref, mshift, epack, wcf, wci, af, ai, bfm, bi):
    info = [neighbour(tab, n) for n in nbrs]
    ga, gb, gc = [[i[0][d] for i in info] for d in range(3)]
    role = [i[1] for i in info]
    w = [i[2] for i in info]
    sext = sext_ref[...]
    ma = shifted_pair(sext, role[0] * ga[0], role[1] * ga[1])
    af[...] = lhs_quad(ma)
    ai[...] = lhs_quad(ma.T)
    mb = shifted_pair(sext, role[0] * gb[0], role[1] * gb[1])
    bfm[...] = lhs_quad(mb)
    bi[...] = lhs_quad(mb.T)
    mc = shifted_pair(sext, role[0] * gc[0], role[1] * gc[1])
    wcf[...] = row_quad(mc.T)
    weight = jnp.where(iota((128, 128), 1) < B, w[0], w[1])
    wci[...] = row_quad(-mc * weight)
    ii, nn = iota((256, 256), 0), iota((256, 256), 1)
    ji, ci = ii // 64, ii % 64
    bo, sn, cn = nn // 128, (nn // 64) % 2, nn % 64
    for s in range(2):
        hit = (sn == s) & (ji == bo + (gb[s] & 1)) & (ci == cn + gc[s])
        mshift[256 * s:256 * s + 256, :] = jnp.where(hit, 1.0, 0.0).astype(bf16)
    epack[...] = jnp.where((ji == bo) & (ci == cn), 1.0, 0.0)[:128].astype(bf16)
    for s, (n_ref, xp) in enumerate(((n0_ref, xp0), (n1_ref, xp1))):
        xp[:, :1024] = jnp.zeros((B, 1024), bf16)
        xp[:, 5120:] = jnp.zeros((B, 1024), bf16)
        sh = jnp.where(iota((B, B), 1) == iota((B, B), 0) + ga[s], 1.0, 0.0).astype(bf16)

        def body(i, _, n_ref=n_ref, xp=xp, sh=sh):
            at = pl.multiple_of(i * 1024, 1024)
            xp[:, pl.ds(at + 1024, 1024)] = dot(sh, n_ref[:, pl.ds(at, 1024)]).astype(bf16)
            return 0
        lax.fori_loop(0, 4, body, 0, unroll=True)
    q0, q1 = 8 + (gb[0] >> 1), 8 + (gb[1] >> 1)

    def stage1(t, _):
        wins, xs = [], []
        for j in range(TB):
            bp = t * TB + j
            l0 = pl.multiple_of((bp + q0) * 128, 128)
            l1 = pl.multiple_of((bp + q1) * 128, 128)
            wins.append(jnp.concatenate([xp0[:, pl.ds(l0, 256)], xp1[:, pl.ds(l1, 256)]], 1))
            xs.append(x_ref[:, pl.ds(pl.multiple_of(bp * 128, 128), 128)])
        y = dot(jnp.concatenate(wins, 0), mshift[...])
        p = dot(jnp.concatenate(xs, 0), epack[...])
        d = y * p
        for j in range(TB):
            for o in range(2):
                y_ref[t * 2 * TB + 2 * j + o] = y[64 * j:64 * j + 64, 128 * o:128 * o + 128].astype(bf16)
        d = jnp.concatenate([d[:, :128], d[:, 128:]], 0)
        d = rows_through(d, wcf[...])
        d = jnp.concatenate([d[64 * (o * TB + j):64 * (o * TB + j) + 64] for j in range(TB) for o in range(2)], 1)
        d = cols_through(af[...], d)
        for k in range(2 * TB):
            z_ref[pl.ds((t * 2 * TB + k) * PITCH, 64), :] = d[:, 128 * k:128 * k + 128]
        return 0
    lax.fori_loop(0, 32 // TB, stage1, 0)

    lev = lev_ref[...]

    def stage2(t, _):
        parts = [z_ref[pl.ds(t * TA + k, 64, stride=PITCH), :] for k in range(TA)]
        d = cols_through(bfm[...], jnp.concatenate(parts, 1))
        g = jnp.concatenate([1.0 / (lev + la_ref[t * TA + k]) for k in range(TA)], 1)
        d = cols_through(bi[...], d * g)
        for k in range(TA):
            z_ref[pl.ds(t * TA + k, 64, stride=PITCH), :] = d[:, 128 * k:128 * k + 128]
        return 0
    lax.fori_loop(0, 64 // TA, stage2, 0)

    lane = iota((B, 128), 1)

    def stage3(t, _):
        parts = [z_ref[pl.ds((t * 2 * TB + k) * PITCH, 64), :] for k in range(2 * TB)]
        d = cols_through(ai[...], jnp.concatenate(parts, 1))
        d = jnp.concatenate([d[:, 128 * k:128 * k + 128] for k in range(2 * TB)], 0)
        d = rows_through(d, wci[...])
        for j in range(TB):
            v = [d[64 * k:64 * k + 64] * y_ref[t * 2 * TB + k].astype(f32) for k in (2 * j, 2 * j + 1)]
            r = jnp.where(lane < B, v[0], v[1]) + pltpu.roll(jnp.where(lane < B, v[1], v[0]), 64, 1)
            at = pl.ds(pl.multiple_of((t * TB + j) * 128, 128), 128)
            out_ref[:, at] = r if first else acc_ref[:, at] + r
        return 0
    lax.fori_loop(0, 32 // TB, stage3, 0)


def pair_call(tab, x, n0, n1, acc, nbrs, TB=16, TA=32):
    first = acc is None
    vm = pl.BlockSpec(memory_space=pltpu.VMEM)
    sm = pl.BlockSpec(memory_space=pltpu.SMEM)
    args = [tab, x, n0, n1] + ([] if first else [acc]) + [jnp.asarray(SEXT), jnp.asarray(LEV), jnp.asarray(LA)]
    specs = [sm, vm, vm, vm] + ([] if first else [vm]) + [vm, vm, sm]

    def body(*refs):
        refs = list(refs)
        if first:
            refs.insert(4, None)
        pair_kernel(TB, TA, first, nbrs, *refs)
    return pl.pallas_call(
        body,
        out_shape=jax.ShapeDtypeStruct((B, B * B), f32),
        in_specs=specs, out_specs=vm,
        scratch_shapes=[
            pltpu.VMEM((B, 6144), bf16), pltpu.VMEM((B, 6144), bf16),
            pltpu.VMEM((B, B, 128), bf16), pltpu.VMEM((B * PITCH + 8, 128), f32),
            pltpu.VMEM((512, 256), bf16), pltpu.VMEM((128, 256), bf16),
            pltpu.VMEM((256, 256), bf16), pltpu.VMEM((256, 256), bf16),
            pltpu.VMEM((128, 256), bf16), pltpu.VMEM((128, 256), bf16),
            pltpu.VMEM((128, 256), bf16), pltpu.VMEM((128, 256), bf16),
        ],
        input_output_aliases={} if first else {4: 0},
        cost_estimate=pl.CostEstimate(flops=10_000_000_000, bytes_accessed=4 << 20, transcendentals=0),
        compiler_params=pltpu.CompilerParams(vmem_limit_bytes=32 << 20),
    )(*args)


def permute(value, target):
    count = lax.axis_size(AXES)
    return lax.ppermute(value, AXES, [(p, target(p) % count) for p in range(count)])


def per_device(orbitals, offsets, pair_list):
    x = orbitals.reshape(B, B * B)
    tab = jnp.concatenate([offsets.T, pair_list.T], 0)
    swap = lambda p: p ^ 1
    near = permute(x, lambda p: p + 2 if p % 2 else p - 2)
    own = permute(x, swap)
    acc = pair_call(tab, x, x, own, None, (0, 1))
    back = permute(x, lambda p: p - 2 if p % 2 else p + 2)
    near, acc = lax.optimization_barrier((near, acc))
    far = permute(near, lambda p: p + 1 if p % 2 else p - 1)
    near_swap = permute(near, swap)
    acc = pair_call(tab, x, near, near_swap, acc, (2, -1))
    back_swap = permute(back, swap)
    acc = pair_call(tab, x, back, back_swap, acc, (-2, 3))
    acc = pair_call(tab, x, far, far, acc, (-3, None))
    return acc.reshape(orbitals.shape)


def solution(mesh):
    in_specs = (P(AXES, None, None), P(), P())
    return jax.shard_map(
        per_device, mesh=mesh, in_specs=in_specs, out_specs=P(AXES, None, None), check_vma=False
    )
```

```python
import jax
import jax.numpy as jnp
import numpy as np
from jax import lax
from jax.experimental import pallas as pl
from jax.experimental.pallas import tpu as pltpu
from jax.sharding import PartitionSpec as P


B = 64
PITCH = 65
AXES = ("blk", "grp")


def constants():
    level = np.arange(1, B + 1, dtype=np.float64)
    sines = np.sqrt(2.0 / (B + 1)) * np.sin(np.pi * level[:, None] * level[None, :] / (B + 1))
    eigen = 2.0 - 2.0 * np.cos(np.pi * level / (B + 1))
    pair = eigen[:, None] + np.tile(eigen, 2)[None, :] + 0.5
    return [np.asarray(t, np.float32) for t in (np.pad(sines, ((0, 0), (32, 32))), pair, np.tile(eigen[:, None], (1, 128)))]


SEXT, LEV, LA = constants()
bf16, f32 = jnp.bfloat16, jnp.float32
OUT = pltpu.VMEM


def split(x):
    hi = x.astype(bf16)
    lo = (x - hi.astype(f32)).astype(bf16)
    return hi, lo


def dot(a, b):
    return jnp.dot(a, b, preferred_element_type=f32)


def iota(shape, dim):
    return lax.broadcasted_iota(jnp.int32, shape, dim)


def shifted_pair(sext, g0, g1):
    lane = iota((B, 128), 1)
    r0 = pltpu.roll(sext, (96 - g0) % 128, 1)
    r1 = pltpu.roll(sext, (160 - g1) % 128, 1)
    return jnp.concatenate([jnp.where(lane < B, r0, 0.0), jnp.where(lane >= B, r1, 0.0)], 0)


def lhs_quad(wide):
    lane = iota((128, 128), 1)
    both = wide + pltpu.roll(wide, 64, 1)
    hi, lo = split(both)
    return jnp.concatenate([hi, lo], 1)


def lhs_halves(wide):
    lane = iota((B, 128), 1)
    block = jnp.where(lane < B, wide[:B], 0.0)
    low = jnp.where(lane < 32, block, 0.0)
    high = pltpu.roll(jnp.where(lane >= 32, block, 0.0), 96, 1)
    both = jnp.concatenate([low, high], 0)
    both = both + pltpu.roll(both, 32, 1)
    hi, lo = split(both)
    whole = (hi.astype(f32) + pltpu.roll(lo.astype(f32), 64, 1)).astype(bf16)
    return jnp.concatenate([whole, jnp.zeros_like(whole)], 1)


def halves_through(lhs, x):
    hi, lo = split(x)
    z = dot(lhs, jnp.concatenate([hi, lo, hi, lo], 0))
    out = []
    lane = iota((32, 128), 1)
    for k in range(x.shape[1] // 128):
        v = z[:, 128 * k:128 * k + 128]
        straight = jnp.where(lane < B, v[:32], v[96:])
        out.append(straight + pltpu.roll(jnp.where(lane < B, v[32:64], v[64:96]), 64, 1))
    return jnp.concatenate(out, 1)


def row_quad(wide):
    hi, lo = split(wide)
    top = jnp.concatenate([hi, lo], 1)
    bottom = jnp.concatenate([hi, jnp.zeros_like(lo)], 1)
    return jnp.concatenate([top, bottom], 0)


def rows_through(x, w):
    hi, lo = split(x)
    z = dot(jnp.concatenate([hi, lo], 1), w)
    return z[:, :128] + z[:, 128:]


def cols_through(lhs, x):
    hi, lo = split(x)
    z = dot(lhs, jnp.concatenate([hi, lo, hi, lo], 0))
    if z.shape[0] == B:
        return z
    lane = iota((B, x.shape[1]), 1)
    return jnp.where(lane % 128 < B, z[:B], z[B:])


def neighbour(tab, nbr):
    count = lax.axis_size(AXES)
    here = lax.axis_index(AXES)
    if not nbr:
        return [0, 0, 0], 0, f32(1.0 if nbr == 0 else 0.0)
    step = jnp.where(here % 2 == 0, nbr, -nbr)
    there = lax.rem(here + step + count, count)
    gaps = [tab[d, here] - tab[d, there] for d in range(3)]
    up = step > 0
    weight = tab[2 + abs(nbr), jnp.where(up, there, here)].astype(f32)
    return gaps, jnp.where(up, 1, 0), weight


ROWS = 1408


def prepare_kernel(calls, tab, sext_ref, *outs):
    sext = sext_ref[...]
    for call, nbrs in enumerate(calls):
        m, steps = outs[2 * call], outs[2 * call + 1]
        lone = nbrs[1] is None
        info = [neighbour(tab, n) for n in (nbrs[:1] * 2 if lone else nbrs)]
        ga, gb, gc = [[i[0][d] for i in info] for d in range(3)]
        role = [i[1] for i in info]
        w = [i[2] for i in info]
        ma = shifted_pair(sext, role[0] * ga[0], role[1] * ga[1])
        m[0:128] = lhs_quad(ma)
        m[128:256] = lhs_quad(ma.T)
        mb = shifted_pair(sext, role[0] * gb[0], role[1] * gb[1])
        m[256:384] = lhs_halves(mb) if lone else lhs_quad(mb)
        m[384:512] = lhs_halves(mb.T) if lone else lhs_quad(mb.T)
        mc = shifted_pair(sext, role[0] * gc[0], role[1] * gc[1])
        m[512:768] = row_quad(mc.T)
        weight = jnp.where(iota((128, 128), 1) < B, w[0], w[1])
        m[768:1024] = row_quad(-mc * weight)
        ii, nn = iota((128, 256), 0), iota((128, 256), 1)
        row, col = iota((B, 256), 0), iota((B, 256), 1)
        for s in range(2):
            hit = ((nn // 64) % 2 == s) & (ii // 64 == nn // 128) & (ii % 64 == nn % 64 + gc[s])
            m[1024 + 128 * s:1152 + 128 * s] = jnp.where(hit, 1.0, 0.0).astype(bf16)
            m[1280 + B * s:1344 + B * s] = jnp.where(col == row + ga[s], 1.0, 0.0).astype(bf16)
            steps[s] = jnp.full((8, 128), gb[s], jnp.int32)


def prepare(tab, calls):
    vm = pl.BlockSpec(memory_space=pltpu.VMEM)
    outs = []
    for _ in calls:
        outs += [OUT((ROWS, 256), bf16), OUT((2, 8, 128), jnp.int32)]
    return pl.pallas_call(
        lambda *refs: prepare_kernel(calls, *refs),
        out_shape=outs, in_specs=[pl.BlockSpec(memory_space=pltpu.SMEM), vm], out_specs=[vm] * len(outs),
        cost_estimate=pl.CostEstimate(flops=3_000_000_000, bytes_accessed=1 << 20, transcendentals=0),
        compiler_params=pltpu.CompilerParams(vmem_limit_bytes=16 << 20),
    )(tab, jnp.asarray(SEXT))


def pair_kernel(TB, TA, first, last, lone, x_hbm, n0_ref, n1_ref, acc_ref, m, steps, lev_ref, la_ref, out_ref,
                x_ref, stage_ref, sems, xp0, xp1, y_ref, z_ref):
    load = pltpu.make_async_copy(x_hbm, x_ref, sems.at[0])
    load.start()
    if first:
        load.wait()
        n0_ref = x_ref
    gb = [jnp.max(steps[s]) for s in range(2)]
    lane = iota((B, 128), 1)
    for s, (n_ref, xp) in enumerate(((n0_ref, xp0), (n1_ref, xp1))[:1 if lone else 2]):
        xp[:, :1024] = jnp.zeros((B, 1024), bf16)
        xp[:, 5120:] = jnp.zeros((B, 1024), bf16)
        odd = gb[s] & 1
        keep = lane < jnp.where(odd == 1, B, 2 * B)
        before = jnp.zeros((B, 128), f32)
        for i in range(4):
            v = dot(m[1280 + B * s:1344 + B * s, :B], n_ref[:, 1024 * i:1024 * i + 1024])
            for j in range(8):
                col = pltpu.roll(v[:, 128 * j:128 * j + 128], 64 * odd, 1)
                at = 1024 * i + 128 * j + 896
                xp[:, at:at + 128] = jnp.where(keep, before, col).astype(bf16)
                before = col
        xp[:, 4992:5120] = jnp.where(keep, before, 0.0).astype(bf16)
    if not first:
        load.wait()
    q0, q1 = 8 + (gb[0] >> 1), 8 + (gb[1] >> 1)
    if lone:
        q1, xp1 = q0 + 16, xp0
    pairs = 16 if lone else 32

    for t in range(pairs // TB):
        wins, even, odds = [], [], []
        for j in range(TB):
            bp = t * TB + j
            l0 = pl.multiple_of((bp + q0) * 128, 128)
            l1 = pl.multiple_of((bp + q1) * 128, 128)
            wins.append(jnp.concatenate([xp0[:, pl.ds(l0, 128)], xp1[:, pl.ds(l1, 128)]], 1))
            v = x_ref[:, 128 * bp:128 * bp + 128].astype(f32)
            u = x_ref[:, 128 * bp + 2048:128 * bp + 2176].astype(f32) if lone else v
            r = pltpu.roll(v, 64, 1)
            even.append(jnp.where(lane < B, v, pltpu.roll(u, 64, 1) if lone else r))
            odds.append(jnp.where(lane < B, r, u))
        y = dot(jnp.concatenate(wins, 0), m[1024:1280])
        for j in range(TB):
            for o in range(2):
                y_ref[t * 2 * TB + 2 * j + o] = y[64 * j:64 * j + 64, 128 * o:128 * o + 128].astype(bf16)
        d = jnp.concatenate([y[:, :128], y[:, 128:]], 0) * jnp.concatenate(even + odds, 0)
        d = rows_through(d, m[512:768])
        d = jnp.concatenate([d[64 * (o * TB + j):64 * (o * TB + j) + 64] for j in range(TB) for o in range(2)], 1)
        d = cols_through(m[0:B if lone else 128], d)
        for k in range(2 * TB):
            at = (t * 2 * TB + k) * PITCH
            z_ref[at:at + 64, :] = d[:, 128 * k:128 * k + 128]

    lev = lev_ref[...]
    if lone:
        lev = jnp.where(iota((32, 128), 1) < B, lev[:32], lev[32:])
    deep = 32 if lone else 64
    through = (lambda a, d: halves_through(m[a:a + 128, :128], d)) if lone else (lambda a, d: cols_through(m[a:a + 128], d))
    for t in range(64 // TA):
        parts = [z_ref[pl.ds(t * TA + k, deep, stride=PITCH), :] for k in range(TA)]
        d = through(256, jnp.concatenate(parts, 1))
        g = jnp.concatenate([1.0 / (lev + la_ref[t * TA + k:t * TA + k + 1, :]) for k in range(TA)], 1)
        d = through(384, d * g)
        for k in range(TA):
            z_ref[pl.ds(t * TA + k, deep, stride=PITCH), :] = d[:, 128 * k:128 * k + 128]

    stores = []
    target = stage_ref if last else out_ref
    for t in range(pairs // TB):
        parts = [z_ref[(t * 2 * TB + k) * PITCH:(t * 2 * TB + k) * PITCH + 64, :] for k in range(2 * TB)]
        d = cols_through(m[128:192 if lone else 256], jnp.concatenate(parts, 1))
        d = jnp.concatenate([d[:, 128 * k:128 * k + 128] for k in range(2 * TB)], 0)
        d = rows_through(d, m[768:1024])
        for j in range(TB):
            v = [d[64 * k:64 * k + 64] * y_ref[t * 2 * TB + k].astype(f32) for k in (2 * j, 2 * j + 1)]
            at = (t * TB + j) * 128
            if lone:
                low = jnp.where(lane < B, v[0], pltpu.roll(v[1], 64, 1))
                high = jnp.where(lane < B, pltpu.roll(v[0], 64, 1), v[1])
                target[:, at:at + 128] = acc_ref[:, at:at + 128] + low
                target[:, at + 2048:at + 2176] = acc_ref[:, at + 2048:at + 2176] + high
            else:
                r = jnp.where(lane < B, v[0], v[1]) + pltpu.roll(jnp.where(lane < B, v[1], v[0]), 64, 1)
                target[:, at:at + 128] = r if first else acc_ref[:, at:at + 128] + r
        if last:
            for at in (t * TB * 128, t * TB * 128 + 2048)[:2 if lone else 1]:
                part = pl.ds(at, TB * 128)
                stores.append(pltpu.make_async_copy(stage_ref.at[:, part], out_ref.at[:, part], sems.at[1 + len(stores)]))
                stores[-1].start()
    for store in stores:
        store.wait()


def pair_call(made, x, n0, n1, acc, last=False, TB=16, TA=32):
    first, lone = acc is None, n1 is None
    TB = min(TB, 8) if lone else TB
    vm = pl.BlockSpec(memory_space=pltpu.VMEM)
    hbm = pl.BlockSpec(memory_space=pl.ANY)
    args = [x] + ([] if first else [n0]) + ([] if lone else [n1]) + ([] if first else [acc])
    args += [*made, jnp.asarray(LEV), jnp.asarray(LA)]
    specs = [hbm] + [vm] * (len(args) - 1)

    def body(*refs):
        refs = list(refs)
        if first:
            refs.insert(1, None)
        if lone:
            refs.insert(2, refs[1])
        if first:
            refs.insert(3, None)
        pair_kernel(TB, TA, first, last, lone, *refs)
    return pl.pallas_call(
        body,
        out_shape=jax.ShapeDtypeStruct((B, B * B), f32) if last else OUT((B, B * B), f32),
        in_specs=specs, out_specs=hbm if last else vm,
        scratch_shapes=[
            pltpu.VMEM((B, B * B), bf16), pltpu.VMEM((B, B * B) if last else (8, 128), f32),
            pltpu.SemaphoreType.DMA((1 + 32 // TB,)),
            pltpu.VMEM((B, 6144), bf16), pltpu.VMEM((B, 6144), bf16),
            pltpu.VMEM((B, B, 128), bf16), pltpu.VMEM((B * PITCH + 8, 128), f32),
        ],
        cost_estimate=pl.CostEstimate(flops=10_000_000_000, bytes_accessed=4 << 20, transcendentals=0),
        compiler_params=pltpu.CompilerParams(vmem_limit_bytes=32 << 20),
    )(*args)


def permute(value, target):
    count = lax.axis_size(AXES)
    return lax.ppermute(value, AXES, [(p, target(p) % count) for p in range(count)])


def per_device(orbitals, offsets, pair_list):
    x = orbitals.reshape(B, B * B)
    tab = jnp.concatenate([offsets.T, pair_list.T], 0)
    swap = lambda p: p ^ 1
    near = permute(x, lambda p: p + 2 if p % 2 else p - 2)
    own = permute(x, swap)
    made = prepare(tab, ((0, 1), (2, -1), (-2, 3), (-3, None)))
    later, mine = lax.optimization_barrier((x, made[0]))
    back = permute(later, lambda p: p - 2 if p % 2 else p + 2)
    acc = pair_call([mine, made[1]], x, x, own, None)
    near, acc = lax.optimization_barrier((near, acc))
    near_swap = permute(near, swap)
    far = permute(near, lambda p: p + 1 if p % 2 else p - 1)
    acc = pair_call(made[2:4], x, near, near_swap, acc)
    back_swap = permute(back, swap)
    acc = pair_call(made[4:6], x, back, back_swap, acc)
    acc = pair_call(made[6:8], x, far, None, acc, last=True)
    return acc.reshape(orbitals.shape)


def solution(mesh):
    in_specs = (P(AXES, None, None), P(), P())
    return jax.shard_map(
        per_device, mesh=mesh, in_specs=in_specs, out_specs=P(AXES, None, None), check_vma=False
    )
```

```python
import jax
import jax.numpy as jnp
import numpy as np
from jax import lax
from jax.experimental import pallas as pl
from jax.experimental.pallas import tpu as pltpu
from jax.sharding import PartitionSpec as P


B = 64
PITCH = 65
AXES = ("blk", "grp")


def constants():
    level = np.arange(1, B + 1, dtype=np.float64)
    sines = np.sqrt(2.0 / (B + 1)) * np.sin(np.pi * level[:, None] * level[None, :] / (B + 1))
    eigen = 2.0 - 2.0 * np.cos(np.pi * level / (B + 1))
    pair = eigen[:, None] + np.tile(eigen, 2)[None, :] + 0.5
    return [np.asarray(t, np.float32) for t in (np.pad(sines, ((0, 0), (32, 32))), pair, np.tile(eigen[:, None], (1, 128)))]


SEXT, LEV, LA = constants()
bf16, f32 = jnp.bfloat16, jnp.float32
OUT = pltpu.VMEM


def split(x):
    hi = x.astype(bf16)
    lo = (x - hi.astype(f32)).astype(bf16)
    return hi, lo


def dot(a, b):
    return jnp.dot(a, b, preferred_element_type=f32)


def iota(shape, dim):
    return lax.broadcasted_iota(jnp.int32, shape, dim)


def shifted_pair(sext, g0, g1):
    lane = iota((B, 128), 1)
    r0 = pltpu.roll(sext, (96 - g0) % 128, 1)
    r1 = pltpu.roll(sext, (160 - g1) % 128, 1)
    return jnp.concatenate([jnp.where(lane < B, r0, 0.0), jnp.where(lane >= B, r1, 0.0)], 0)


def lhs_quad(wide):
    lane = iota((128, 128), 1)
    both = wide + pltpu.roll(wide, 64, 1)
    hi, lo = split(both)
    return jnp.concatenate([hi, lo], 1)


def lhs_halves(wide):
    lane = iota((B, 128), 1)
    block = jnp.where(lane < B, wide[:B], 0.0)
    low = jnp.where(lane < 32, block, 0.0)
    high = pltpu.roll(jnp.where(lane >= 32, block, 0.0), 96, 1)
    both = jnp.concatenate([low, high], 0)
    both = both + pltpu.roll(both, 32, 1)
    hi, lo = split(both)
    whole = (hi.astype(f32) + pltpu.roll(lo.astype(f32), 64, 1)).astype(bf16)
    return jnp.concatenate([whole, jnp.zeros_like(whole)], 1)


def halves_through(lhs, x):
    hi, lo = split(x)
    z = dot(lhs, jnp.concatenate([hi, lo, hi, lo], 0))
    out = []
    lane = iota((32, 128), 1)
    for k in range(x.shape[1] // 128):
        v = z[:, 128 * k:128 * k + 128]
        straight = jnp.where(lane < B, v[:32], v[96:])
        out.append(straight + pltpu.roll(jnp.where(lane < B, v[32:64], v[64:96]), 64, 1))
    return jnp.concatenate(out, 1)


def row_quad(wide):
    hi, lo = split(wide)
    top = jnp.concatenate([hi, lo], 1)
    bottom = jnp.concatenate([hi, jnp.zeros_like(lo)], 1)
    return jnp.concatenate([top, bottom], 0)


def rows_through(x, w):
    hi, lo = split(x)
    z = dot(jnp.concatenate([hi, lo], 1), w)
    return z[:, :128] + z[:, 128:]


def cols_through(lhs, x):
    hi, lo = split(x)
    z = dot(lhs[:, :192], jnp.concatenate([hi, lo, hi], 0))
    if z.shape[0] == B:
        return z
    lane = iota((B, x.shape[1]), 1)
    return jnp.where(lane % 128 < B, z[:B], z[B:])


def neighbour(tab, nbr):
    count = lax.axis_size(AXES)
    here = lax.axis_index(AXES)
    if not nbr:
        return [0, 0, 0], 0, f32(1.0 if nbr == 0 else 0.0)
    step = jnp.where(here % 2 == 0, nbr, -nbr)
    there = lax.rem(here + step + count, count)
    gaps = [tab[d, here] - tab[d, there] for d in range(3)]
    up = step > 0
    weight = tab[2 + abs(nbr), jnp.where(up, there, here)].astype(f32)
    return gaps, jnp.where(up, 1, 0), weight


ROWS = 1408


def prepare_kernel(calls, tab, sext_ref, *outs):
    sext = sext_ref[...]
    for call, nbrs in enumerate(calls):
        m, steps = outs[2 * call], outs[2 * call + 1]
        lone = nbrs[1] is None
        info = [neighbour(tab, n) for n in (nbrs[:1] * 2 if lone else nbrs)]
        ga, gb, gc = [[i[0][d] for i in info] for d in range(3)]
        role = [i[1] for i in info]
        w = [i[2] for i in info]
        ma = shifted_pair(sext, role[0] * ga[0], role[1] * ga[1])
        m[0:128] = lhs_quad(ma)
        m[128:256] = lhs_quad(ma.T)
        mb = shifted_pair(sext, role[0] * gb[0], role[1] * gb[1])
        m[256:384] = lhs_halves(mb) if lone else lhs_quad(mb)
        m[384:512] = lhs_halves(mb.T) if lone else lhs_quad(mb.T)
        mc = shifted_pair(sext, role[0] * gc[0], role[1] * gc[1])
        m[512:768] = row_quad(mc.T)
        weight = jnp.where(iota((128, 128), 1) < B, w[0], w[1])
        m[768:1024] = row_quad(-mc * weight)
        ii, nn = iota((128, 256), 0), iota((128, 256), 1)
        row, col = iota((B, 256), 0), iota((B, 256), 1)
        for s in range(2):
            hit = ((nn // 64) % 2 == s) & (ii // 64 == nn // 128) & (ii % 64 == nn % 64 + gc[s])
            m[1024 + 128 * s:1152 + 128 * s] = jnp.where(hit, 1.0, 0.0).astype(bf16)
            m[1280 + B * s:1344 + B * s] = jnp.where(col == row + ga[s], 1.0, 0.0).astype(bf16)
            steps[s] = jnp.full((8, 128), gb[s], jnp.int32)


def prepare(tab, calls):
    vm = pl.BlockSpec(memory_space=pltpu.VMEM)
    outs = []
    for _ in calls:
        outs += [OUT((ROWS, 256), bf16), OUT((2, 8, 128), jnp.int32)]
    return pl.pallas_call(
        lambda *refs: prepare_kernel(calls, *refs),
        out_shape=outs, in_specs=[pl.BlockSpec(memory_space=pltpu.SMEM), vm], out_specs=[vm] * len(outs),
        cost_estimate=pl.CostEstimate(flops=3_000_000_000, bytes_accessed=1 << 20, transcendentals=0),
        compiler_params=pltpu.CompilerParams(vmem_limit_bytes=16 << 20),
    )(tab, jnp.asarray(SEXT))


def staggered(count, steps):
    values = {}
    for i in range(count + 2 * (len(steps) - 1)):
        for j, step in enumerate(steps):
            t = i - 2 * j
            if 0 <= t < count:
                values[t] = step(t, values.pop(t, None))


def pair_kernel(TB, TA, first, last, lone, x_hbm, n0_ref, n1_ref, acc_ref, m, steps, lev_ref, la_ref, out_ref,
                x_ref, stage_ref, sems, xp0, xp1, y_ref, z_ref):
    load = pltpu.make_async_copy(x_hbm, x_ref, sems.at[0])
    load.start()
    if first:
        load.wait()
        n0_ref = x_ref
    gb = [jnp.max(steps[s]) for s in range(2)]
    lane = iota((B, 128), 1)
    for s, (n_ref, xp) in enumerate(((n0_ref, xp0), (n1_ref, xp1))[:1 if lone else 2]):
        xp[:, :1024] = jnp.zeros((B, 1024), bf16)
        xp[:, 5120:] = jnp.zeros((B, 1024), bf16)
        odd = gb[s] & 1
        keep = lane < jnp.where(odd == 1, B, 2 * B)
        before = jnp.zeros((B, 128), f32)
        for i in range(4):
            v = dot(m[1280 + B * s:1344 + B * s, :B], n_ref[:, 1024 * i:1024 * i + 1024])
            for j in range(8):
                col = pltpu.roll(v[:, 128 * j:128 * j + 128], 64 * odd, 1)
                at = 1024 * i + 128 * j + 896
                xp[:, at:at + 128] = jnp.where(keep, before, col).astype(bf16)
                before = col
        xp[:, 4992:5120] = jnp.where(keep, before, 0.0).astype(bf16)
    if not first:
        load.wait()
    q0, q1 = 8 + (gb[0] >> 1), 8 + (gb[1] >> 1)
    if lone:
        q1, xp1 = q0 + 16, xp0
    pairs = 16 if lone else 32

    def moved(t, _):
        wins = []
        for j in range(TB):
            bp = t * TB + j
            l0 = pl.multiple_of((bp + q0) * 128, 128)
            l1 = pl.multiple_of((bp + q1) * 128, 128)
            wins.append(jnp.concatenate([xp0[:, pl.ds(l0, 128)], xp1[:, pl.ds(l1, 128)]], 1))
        return dot(jnp.concatenate(wins, 0), m[1024:1280])

    def density(t, y):
        even, odds = [], []
        for j in range(TB):
            bp = t * TB + j
            v = x_ref[:, 128 * bp:128 * bp + 128].astype(f32)
            u = x_ref[:, 128 * bp + 2048:128 * bp + 2176].astype(f32) if lone else v
            r = pltpu.roll(v, 64, 1)
            even.append(jnp.where(lane < B, v, pltpu.roll(u, 64, 1) if lone else r))
            odds.append(jnp.where(lane < B, r, u))
            for o in range(2):
                y_ref[t * 2 * TB + 2 * j + o] = y[64 * j:64 * j + 64, 128 * o:128 * o + 128].astype(bf16)
        d = jnp.concatenate([y[:, :128], y[:, 128:]], 0) * jnp.concatenate(even + odds, 0)
        return rows_through(d, m[512:768])

    def first_forward(t, d):
        d = jnp.concatenate([d[64 * (o * TB + j):64 * (o * TB + j) + 64] for j in range(TB) for o in range(2)], 1)
        d = cols_through(m[0:B if lone else 128], d)
        for k in range(2 * TB):
            at = (t * 2 * TB + k) * PITCH
            z_ref[at:at + 64, :] = d[:, 128 * k:128 * k + 128]

    staggered(pairs // TB, (moved, density, first_forward))

    lev = lev_ref[...]
    if lone:
        lev = jnp.where(iota((32, 128), 1) < B, lev[:32], lev[32:])
    deep = 32 if lone else 64
    through = (lambda a, d: halves_through(m[a:a + 128, :128], d)) if lone else (lambda a, d: cols_through(m[a:a + 128], d))

    def second_forward(t, _):
        parts = [z_ref[pl.ds(t * TA + k, deep, stride=PITCH), :] for k in range(TA)]
        d = through(256, jnp.concatenate(parts, 1))
        g = jnp.concatenate([1.0 / (lev + la_ref[t * TA + k:t * TA + k + 1, :]) for k in range(TA)], 1)
        return d * g

    def second_back(t, d):
        d = through(384, d)
        for k in range(TA):
            z_ref[pl.ds(t * TA + k, deep, stride=PITCH), :] = d[:, 128 * k:128 * k + 128]

    staggered(64 // TA, (second_forward, second_back))

    stores = []
    target = stage_ref if last else out_ref

    def first_back(t, _):
        parts = [z_ref[(t * 2 * TB + k) * PITCH:(t * 2 * TB + k) * PITCH + 64, :] for k in range(2 * TB)]
        return cols_through(m[128:192 if lone else 256], jnp.concatenate(parts, 1))

    def last_back(t, d):
        d = jnp.concatenate([d[:, 128 * k:128 * k + 128] for k in range(2 * TB)], 0)
        d = rows_through(d, m[768:1024])
        for j in range(TB):
            v = [d[64 * k:64 * k + 64] * y_ref[t * 2 * TB + k].astype(f32) for k in (2 * j, 2 * j + 1)]
            at = (t * TB + j) * 128
            if lone:
                low = jnp.where(lane < B, v[0], pltpu.roll(v[1], 64, 1))
                high = jnp.where(lane < B, pltpu.roll(v[0], 64, 1), v[1])
                target[:, at:at + 128] = acc_ref[:, at:at + 128] + low
                target[:, at + 2048:at + 2176] = acc_ref[:, at + 2048:at + 2176] + high
            else:
                r = jnp.where(lane < B, v[0], v[1]) + pltpu.roll(jnp.where(lane < B, v[1], v[0]), 64, 1)
                target[:, at:at + 128] = r if first else acc_ref[:, at:at + 128] + r
        if last:
            for at in (t * TB * 128, t * TB * 128 + 2048)[:2 if lone else 1]:
                part = pl.ds(at, TB * 128)
                stores.append(pltpu.make_async_copy(stage_ref.at[:, part], out_ref.at[:, part], sems.at[1 + len(stores)]))
                stores[-1].start()

    staggered(pairs // TB, (first_back, last_back))
    for store in stores:
        store.wait()


def pair_call(made, x, n0, n1, acc, last=False, TB=4, TA=8, LB=4):
    first, lone = acc is None, n1 is None
    TB = min(TB, LB) if lone else TB
    vm = pl.BlockSpec(memory_space=pltpu.VMEM)
    hbm = pl.BlockSpec(memory_space=pl.ANY)
    args = [x] + ([] if first else [n0]) + ([] if lone else [n1]) + ([] if first else [acc])
    args += [*made, jnp.asarray(LEV), jnp.asarray(LA)]
    specs = [hbm] + [vm] * (len(args) - 1)

    def body(*refs):
        refs = list(refs)
        if first:
            refs.insert(1, None)
        if lone:
            refs.insert(2, refs[1])
        if first:
            refs.insert(3, None)
        pair_kernel(TB, TA, first, last, lone, *refs)

    return pl.pallas_call(
        body,
        out_shape=jax.ShapeDtypeStruct((B, B * B), f32) if last else OUT((B, B * B), f32),
        in_specs=specs, out_specs=hbm if last else vm,
        scratch_shapes=[
            pltpu.VMEM((B, B * B), bf16), pltpu.VMEM((B, B * B) if last else (8, 128), f32),
            pltpu.SemaphoreType.DMA((1 + 32 // TB,)),
            pltpu.VMEM((B, 6144), bf16), pltpu.VMEM((B, 6144), bf16),
            pltpu.VMEM((B, B, 128), bf16), pltpu.VMEM((B * PITCH + 8, 128), f32),
        ],
        cost_estimate=pl.CostEstimate(flops=10_000_000_000, bytes_accessed=4 << 20, transcendentals=0),
        compiler_params=pltpu.CompilerParams(vmem_limit_bytes=32 << 20),
    )(*args)


def permute(value, target):
    count = lax.axis_size(AXES)
    return lax.ppermute(value, AXES, [(p, target(p) % count) for p in range(count)])


def per_device(orbitals, offsets, pair_list):
    x = orbitals.reshape(B, B * B)
    tab = jnp.concatenate([offsets.T, pair_list.T], 0)
    swap = lambda p: p ^ 1
    near = permute(x, lambda p: p + 2 if p % 2 else p - 2)
    own = permute(x, swap)
    made = prepare(tab, ((0, 1), (2, -1), (-2, 3), (-3, None)))
    later, mine = lax.optimization_barrier((x, made[0]))
    back = permute(later, lambda p: p - 2 if p % 2 else p + 2)
    acc = pair_call([mine, made[1]], x, x, own, None)
    near, acc = lax.optimization_barrier((near, acc))
    near_swap = permute(near, swap)
    far = permute(near, lambda p: p + 1 if p % 2 else p - 1)
    acc = pair_call(made[2:4], x, near, near_swap, acc)
    back_swap = permute(back, swap)
    acc = pair_call(made[4:6], x, back, back_swap, acc)
    acc = pair_call(made[6:8], x, far, None, acc, last=True)
    return acc.reshape(orbitals.shape)


def solution(mesh):
    in_specs = (P(AXES, None, None), P(), P())
    return jax.shard_map(
        per_device, mesh=mesh, in_specs=in_specs, out_specs=P(AXES, None, None), check_vma=False
    )
```

```python
import jax
import jax.numpy as jnp
import numpy as np
from jax import lax
from jax.experimental import pallas as pl
from jax.experimental.pallas import tpu as pltpu
from jax.sharding import PartitionSpec as P


B = 64
PITCH = 65
AXES = ("blk", "grp")


def constants():
    level = np.arange(1, B + 1, dtype=np.float64)
    sines = np.sqrt(2.0 / (B + 1)) * np.sin(np.pi * level[:, None] * level[None, :] / (B + 1))
    eigen = 2.0 - 2.0 * np.cos(np.pi * level / (B + 1))
    pair = eigen[:, None] + np.tile(eigen, 2)[None, :] + 0.5
    return [np.asarray(t, np.float32) for t in (np.pad(sines, ((0, 0), (32, 32))), pair, np.tile(eigen[:, None], (1, 128)))]


SEXT, LEV, LA = constants()
bf16, f32 = jnp.bfloat16, jnp.float32
OUT = pltpu.VMEM


def split(x):
    hi = x.astype(bf16)
    lo = (x - hi.astype(f32)).astype(bf16)
    return hi, lo


def dot(a, b):
    return jnp.dot(a, b, preferred_element_type=f32)


def iota(shape, dim):
    return lax.broadcasted_iota(jnp.int32, shape, dim)


def shifted_pair(sext, g0, g1):
    lane = iota((B, 128), 1)
    r0 = pltpu.roll(sext, (96 - g0) % 128, 1)
    r1 = pltpu.roll(sext, (160 - g1) % 128, 1)
    return jnp.concatenate([jnp.where(lane < B, r0, 0.0), jnp.where(lane >= B, r1, 0.0)], 0)


def lhs_quad(wide):
    lane = iota((128, 128), 1)
    both = wide + pltpu.roll(wide, 64, 1)
    hi, lo = split(both)
    return jnp.concatenate([hi, lo], 1)


def lhs_halves(wide):
    lane = iota((B, 128), 1)
    block = jnp.where(lane < B, wide[:B], 0.0)
    low = jnp.where(lane < 32, block, 0.0)
    high = pltpu.roll(jnp.where(lane >= 32, block, 0.0), 96, 1)
    both = jnp.concatenate([low, high], 0)
    both = both + pltpu.roll(both, 32, 1)
    hi, lo = split(both)
    whole = (hi.astype(f32) + pltpu.roll(lo.astype(f32), 64, 1)).astype(bf16)
    return jnp.concatenate([whole, jnp.zeros_like(whole)], 1)


def halves_through(lhs, x):
    hi, lo = split(x)
    z = dot(lhs, jnp.concatenate([hi, lo, hi, lo], 0))
    out = []
    lane = iota((32, 128), 1)
    for k in range(x.shape[1] // 128):
        v = z[:, 128 * k:128 * k + 128]
        straight = jnp.where(lane < B, v[:32], v[96:])
        out.append(straight + pltpu.roll(jnp.where(lane < B, v[32:64], v[64:96]), 64, 1))
    return jnp.concatenate(out, 1)


def row_quad(wide):
    hi, lo = split(wide)
    top = jnp.concatenate([hi, lo], 1)
    bottom = jnp.concatenate([hi, jnp.zeros_like(lo)], 1)
    return jnp.concatenate([top, bottom], 0)


def rows_through(x, w):
    hi, lo = split(x)
    z = dot(jnp.concatenate([hi, lo], 1), w)
    return z[:, :128] + z[:, 128:]


def cols_through(lhs, x):
    hi, lo = split(x)
    z = dot(lhs[:, :192], jnp.concatenate([hi, lo, hi], 0))
    if z.shape[0] == B:
        return z
    lane = iota((B, x.shape[1]), 1)
    return jnp.where(lane % 128 < B, z[:B], z[B:])


def neighbour(tab, nbr):
    count = lax.axis_size(AXES)
    here = lax.axis_index(AXES)
    if not nbr:
        return [0, 0, 0], 0, f32(1.0 if nbr == 0 else 0.0)
    step = jnp.where(here % 2 == 0, nbr, -nbr)
    there = lax.rem(here + step + count, count)
    gaps = [tab[d, here] - tab[d, there] for d in range(3)]
    up = step > 0
    weight = tab[2 + abs(nbr), jnp.where(up, there, here)].astype(f32)
    return gaps, jnp.where(up, 1, 0), weight


ROWS = 1408


def prepare_kernel(calls, tab, sext_ref, *outs):
    sext = sext_ref[...]
    for call, nbrs in enumerate(calls):
        m, steps = outs[2 * call], outs[2 * call + 1]
        lone = nbrs[1] is None
        info = [neighbour(tab, n) for n in (nbrs[:1] * 2 if lone else nbrs)]
        ga, gb, gc = [[i[0][d] for i in info] for d in range(3)]
        role = [i[1] for i in info]
        w = [i[2] for i in info]
        ma = shifted_pair(sext, role[0] * ga[0], role[1] * ga[1])
        m[0:128] = lhs_quad(ma)
        m[128:256] = lhs_quad(ma.T)
        mb = shifted_pair(sext, role[0] * gb[0], role[1] * gb[1])
        m[256:384] = lhs_halves(mb) if lone else lhs_quad(mb)
        m[384:512] = lhs_halves(mb.T) if lone else lhs_quad(mb.T)
        mc = shifted_pair(sext, role[0] * gc[0], role[1] * gc[1])
        m[512:768] = row_quad(mc.T)
        weight = jnp.where(iota((128, 128), 1) < B, w[0], w[1])
        m[768:1024] = row_quad(-mc * weight)
        ii, nn = iota((128, 256), 0), iota((128, 256), 1)
        row, col = iota((B, 256), 0), iota((B, 256), 1)
        for s in range(2):
            hit = ((nn // 64) % 2 == s) & (ii // 64 == nn // 128) & (ii % 64 == nn % 64 + gc[s])
            m[1024 + 128 * s:1152 + 128 * s] = jnp.where(hit, 1.0, 0.0).astype(bf16)
            m[1280 + B * s:1344 + B * s] = jnp.where(col == row + ga[s], 1.0, 0.0).astype(bf16)
            steps[s] = jnp.full((8, 128), gb[s], jnp.int32)


def prepare(tab, calls):
    vm = pl.BlockSpec(memory_space=pltpu.VMEM)
    outs = []
    for _ in calls:
        outs += [OUT((ROWS, 256), bf16), OUT((2, 8, 128), jnp.int32)]
    return pl.pallas_call(
        lambda *refs: prepare_kernel(calls, *refs),
        out_shape=outs, in_specs=[pl.BlockSpec(memory_space=pltpu.SMEM), vm], out_specs=[vm] * len(outs),
        cost_estimate=pl.CostEstimate(flops=3_000_000_000, bytes_accessed=1 << 20, transcendentals=0),
        compiler_params=pltpu.CompilerParams(vmem_limit_bytes=16 << 20),
    )(tab, jnp.asarray(SEXT))


def staggered(count, steps):
    values = {}
    for i in range(count + 2 * (len(steps) - 1)):
        for j, step in enumerate(steps):
            t = i - 2 * j
            if 0 <= t < count:
                values[t] = step(t, values.pop(t, None))


def pair_kernel(TB, TA, first, last, lone, x_hbm, n0_ref, n1_ref, acc_ref, m, steps, lev_ref, la_ref, out_ref,
                x_ref, stage_ref, sems, xp0, xp1, y_ref, z_ref):
    load = pltpu.make_async_copy(x_hbm, x_ref, sems.at[0])
    load.start()
    if first:
        load.wait()
        n0_ref = x_ref
    gb = [jnp.max(steps[s]) for s in range(2)]
    lane = iota((B, 128), 1)
    for s, (n_ref, xp) in enumerate(((n0_ref, xp0), (n1_ref, xp1))[:1 if lone else 2]):
        xp[:, :1024] = jnp.zeros((B, 1024), bf16)
        xp[:, 5120:] = jnp.zeros((B, 1024), bf16)
        odd = gb[s] & 1
        keep = lane < jnp.where(odd == 1, B, 2 * B)
        before = jnp.zeros((B, 128), f32)
        for i in range(4):
            v = dot(m[1280 + B * s:1344 + B * s, :B], n_ref[:, 1024 * i:1024 * i + 1024])
            for j in range(8):
                col = pltpu.roll(v[:, 128 * j:128 * j + 128], 64 * odd, 1)
                at = 1024 * i + 128 * j + 896
                xp[:, at:at + 128] = jnp.where(keep, before, col).astype(bf16)
                before = col
        xp[:, 4992:5120] = jnp.where(keep, before, 0.0).astype(bf16)
    if not first:
        load.wait()
    q0, q1 = 8 + (gb[0] >> 1), 8 + (gb[1] >> 1)
    if lone:
        q1, xp1 = q0 + 16, xp0
    pairs = 16 if lone else 32

    def moved(t, _):
        wins = []
        for j in range(TB):
            bp = t * TB + j
            l0 = pl.multiple_of((bp + q0) * 128, 128)
            l1 = pl.multiple_of((bp + q1) * 128, 128)
            wins.append(jnp.concatenate([xp0[:, pl.ds(l0, 128)], xp1[:, pl.ds(l1, 128)]], 1))
        return dot(jnp.concatenate(wins, 0), m[1024:1280])

    def density(t, y):
        even, odds = [], []
        for j in range(TB):
            bp = t * TB + j
            v = x_ref[:, 128 * bp:128 * bp + 128].astype(f32)
            u = x_ref[:, 128 * bp + 2048:128 * bp + 2176].astype(f32) if lone else v
            r = pltpu.roll(v, 64, 1)
            even.append(jnp.where(lane < B, v, pltpu.roll(u, 64, 1) if lone else r))
            odds.append(jnp.where(lane < B, r, u))
            for o in range(2):
                y_ref[t * 2 * TB + 2 * j + o] = y[64 * j:64 * j + 64, 128 * o:128 * o + 128].astype(bf16)
        d = jnp.concatenate([y[:, :128], y[:, 128:]], 0) * jnp.concatenate(even + odds, 0)
        return rows_through(d, m[512:768])

    def first_forward(t, d):
        d = jnp.concatenate([d[64 * (o * TB + j):64 * (o * TB + j) + 64] for j in range(TB) for o in range(2)], 1)
        d = cols_through(m[0:B if lone else 128], d)
        for k in range(2 * TB):
            at = (t * 2 * TB + k) * PITCH
            z_ref[at:at + 64, :] = d[:, 128 * k:128 * k + 128]

    staggered(pairs // TB, (moved, density, first_forward))

    lev = lev_ref[...]
    if lone:
        lev = jnp.where(iota((32, 128), 1) < B, lev[:32], lev[32:])
    deep = 32 if lone else 64
    through = (lambda a, d: halves_through(m[a:a + 128, :128], d)) if lone else (lambda a, d: cols_through(m[a:a + 128], d))

    def second_forward(t, _):
        parts = [z_ref[pl.ds(t * TA + k, deep, stride=PITCH), :] for k in range(TA)]
        d = through(256, jnp.concatenate(parts, 1))
        g = jnp.concatenate([1.0 / (lev + la_ref[t * TA + k:t * TA + k + 1, :]) for k in range(TA)], 1)
        return d * g

    def second_back(t, d):
        d = through(384, d)
        for k in range(TA):
            z_ref[pl.ds(t * TA + k, deep, stride=PITCH), :] = d[:, 128 * k:128 * k + 128]

    staggered(64 // TA, (second_forward, second_back))

    stores = []
    target = stage_ref if last else out_ref

    def first_back(t, _):
        parts = [z_ref[(t * 2 * TB + k) * PITCH:(t * 2 * TB + k) * PITCH + 64, :] for k in range(2 * TB)]
        return cols_through(m[128:192 if lone else 256], jnp.concatenate(parts, 1))

    def last_back(t, d):
        d = jnp.concatenate([d[:, 128 * k:128 * k + 128] for k in range(2 * TB)], 0)
        d = rows_through(d, m[768:1024])
        for j in range(TB):
            v = [d[64 * k:64 * k + 64] * y_ref[t * 2 * TB + k].astype(f32) for k in (2 * j, 2 * j + 1)]
            at = (t * TB + j) * 128
            if lone:
                low = jnp.where(lane < B, v[0], pltpu.roll(v[1], 64, 1))
                high = jnp.where(lane < B, pltpu.roll(v[0], 64, 1), v[1])
                target[:, at:at + 128] = acc_ref[:, at:at + 128] + low
                target[:, at + 2048:at + 2176] = acc_ref[:, at + 2048:at + 2176] + high
            else:
                r = jnp.where(lane < B, v[0], v[1]) + pltpu.roll(jnp.where(lane < B, v[1], v[0]), 64, 1)
                target[:, at:at + 128] = r if first else acc_ref[:, at:at + 128] + r
        if last:
            for at in (t * TB * 128, t * TB * 128 + 2048)[:2 if lone else 1]:
                part = pl.ds(at, TB * 128)
                stores.append(pltpu.make_async_copy(stage_ref.at[:, part], out_ref.at[:, part], sems.at[1 + len(stores)]))
                stores[-1].start()

    staggered(pairs // TB, (first_back, last_back))
    for store in stores:
        store.wait()


def pair_call(made, x, n0, n1, acc, last=False, TB=4, TA=8, LB=4):
    first, lone = acc is None, n1 is None
    TB = min(TB, LB) if lone else TB
    vm = pl.BlockSpec(memory_space=pltpu.VMEM)
    hbm = pl.BlockSpec(memory_space=pl.ANY)
    args = [x] + ([] if first else [n0]) + ([] if lone else [n1]) + ([] if first else [acc])
    args += [*made, jnp.asarray(LEV), jnp.asarray(LA)]
    specs = [hbm] + [vm] * (len(args) - 1)

    def body(*refs):
        refs = list(refs)
        if first:
            refs.insert(1, None)
        if lone:
            refs.insert(2, refs[1])
        if first:
            refs.insert(3, None)
        pair_kernel(TB, TA, first, last, lone, *refs)

    return pl.pallas_call(
        body,
        out_shape=jax.ShapeDtypeStruct((B, B * B), f32) if last else OUT((B, B * B), f32),
        in_specs=specs, out_specs=hbm if last else vm,
        scratch_shapes=[
            pltpu.VMEM((B, B * B), bf16), pltpu.VMEM((B, B * B) if last else (8, 128), f32),
            pltpu.SemaphoreType.DMA((1 + 32 // TB,)),
            pltpu.VMEM((B, 6144), bf16), pltpu.VMEM((B, 6144), bf16),
            pltpu.VMEM((B, B, 128), bf16), pltpu.VMEM((B * PITCH + 8, 128), f32),
        ],
        cost_estimate=pl.CostEstimate(flops=10_000_000_000, bytes_accessed=4 << 20, transcendentals=0),
        compiler_params=pltpu.CompilerParams(vmem_limit_bytes=32 << 20),
    )(*args)


def permute(value, target):
    count = lax.axis_size(AXES)
    return lax.ppermute(value, AXES, [(p, target(p) % count) for p in range(count)])


def per_device(orbitals, offsets, pair_list):
    x = orbitals.reshape(B, B * B)
    tab = jnp.concatenate([offsets.T, pair_list.T], 0)
    swap = lambda p: p ^ 1
    near = permute(x, lambda p: p + 2 if p % 2 else p - 2)
    own = permute(x, swap)
    made = prepare(tab, ((0, 1), (2, None), (-1, -2), (3, -3)))
    later, mine = lax.optimization_barrier((x, made[0]))
    back = permute(later, lambda p: p - 2 if p % 2 else p + 2)
    acc = pair_call([mine, made[1]], x, x, own, None)
    near, acc = lax.optimization_barrier((near, acc))
    far = permute(near, lambda p: p + 1 if p % 2 else p - 1)
    near_swap = permute(near, swap)
    acc = pair_call(made[2:4], x, near, None, acc)
    back, acc = lax.optimization_barrier((back, acc))
    back_swap = permute(back, swap)
    acc = pair_call(made[4:6], x, near_swap, back, acc)
    acc = pair_call(made[6:8], x, back_swap, far, acc, last=True)
    return acc.reshape(orbitals.shape)


def solution(mesh):
    in_specs = (P(AXES, None, None), P(), P())
    return jax.shard_map(
        per_device, mesh=mesh, in_specs=in_specs, out_specs=P(AXES, None, None), check_vma=False
    )
```

```python
import jax
import jax.numpy as jnp
import numpy as np
from jax import lax
from jax.experimental import pallas as pl
from jax.experimental.pallas import tpu as pltpu
from jax.sharding import PartitionSpec as P


B = 64
PITCH = 65
AXES = ("blk", "grp")


def constants():
    level = np.arange(1, B + 1, dtype=np.float64)
    sines = np.sqrt(2.0 / (B + 1)) * np.sin(np.pi * level[:, None] * level[None, :] / (B + 1))
    eigen = 2.0 - 2.0 * np.cos(np.pi * level / (B + 1))
    pair = eigen[:, None] + np.tile(eigen, 2)[None, :] + 0.5
    return [np.asarray(t, np.float32) for t in (np.pad(sines, ((0, 0), (32, 32))), pair, np.tile(eigen[:, None], (1, 128)))]


SEXT, LEV, LA = constants()
bf16, f32 = jnp.bfloat16, jnp.float32
OUT = pltpu.VMEM


def split(x):
    hi = x.astype(bf16)
    lo = (x - hi.astype(f32)).astype(bf16)
    return hi, lo


def dot(a, b):
    return jnp.dot(a, b, preferred_element_type=f32)


def iota(shape, dim):
    return lax.broadcasted_iota(jnp.int32, shape, dim)


def shifted_pair(sext, g0, g1):
    lane = iota((B, 128), 1)
    r0 = pltpu.roll(sext, (96 - g0) % 128, 1)
    r1 = pltpu.roll(sext, (160 - g1) % 128, 1)
    return jnp.concatenate([jnp.where(lane < B, r0, 0.0), jnp.where(lane >= B, r1, 0.0)], 0)


def lhs_quad(wide):
    lane = iota((128, 128), 1)
    both = wide + pltpu.roll(wide, 64, 1)
    hi, lo = split(both)
    return jnp.concatenate([hi, lo], 1)


def lhs_halves(wide):
    lane = iota((B, 128), 1)
    block = jnp.where(lane < B, wide[:B], 0.0)
    low = jnp.where(lane < 32, block, 0.0)
    high = pltpu.roll(jnp.where(lane >= 32, block, 0.0), 96, 1)
    both = jnp.concatenate([low, high], 0)
    both = both + pltpu.roll(both, 32, 1)
    hi, lo = split(both)
    whole = (hi.astype(f32) + pltpu.roll(lo.astype(f32), 64, 1)).astype(bf16)
    return jnp.concatenate([whole, jnp.zeros_like(whole)], 1)


def halves_through(lhs, x):
    hi, lo = split(x)
    z = dot(lhs, jnp.concatenate([hi, lo, hi, lo], 0))
    out = []
    lane = iota((32, 128), 1)
    for k in range(x.shape[1] // 128):
        v = z[:, 128 * k:128 * k + 128]
        straight = jnp.where(lane < B, v[:32], v[96:])
        out.append(straight + pltpu.roll(jnp.where(lane < B, v[32:64], v[64:96]), 64, 1))
    return jnp.concatenate(out, 1)


def row_quad(wide):
    hi, lo = split(wide)
    top = jnp.concatenate([hi, lo], 1)
    bottom = jnp.concatenate([hi, jnp.zeros_like(lo)], 1)
    return jnp.concatenate([top, bottom], 0)


def rows_through(x, w):
    hi, lo = split(x)
    z = dot(jnp.concatenate([hi, lo], 1), w)
    return z[:, :128] + z[:, 128:]


def cols_through(lhs, x):
    hi, lo = split(x)
    z = dot(lhs[:, :192], jnp.concatenate([hi, lo, hi], 0))
    if z.shape[0] == B:
        return z
    lane = iota((B, x.shape[1]), 1)
    return jnp.where(lane % 128 < B, z[:B], z[B:])


def neighbour(tab, nbr):
    count = lax.axis_size(AXES)
    here = lax.axis_index(AXES)
    if not nbr:
        return [0, 0, 0], 0, f32(1.0 if nbr == 0 else 0.0)
    step = jnp.where(here % 2 == 0, nbr, -nbr)
    there = lax.rem(here + step + count, count)
    gaps = [tab[d, here] - tab[d, there] for d in range(3)]
    up = step > 0
    weight = tab[2 + abs(nbr), jnp.where(up, there, here)].astype(f32)
    return gaps, jnp.where(up, 1, 0), weight


ROWS = 1408


def prepare_kernel(calls, tab, sext_ref, *outs):
    sext = sext_ref[...]
    for call, nbrs in enumerate(calls):
        m, steps = outs[2 * call], outs[2 * call + 1]
        lone = nbrs[1] is None
        info = [neighbour(tab, n) for n in (nbrs[:1] * 2 if lone else nbrs)]
        ga, gb, gc = [[i[0][d] for i in info] for d in range(3)]
        role = [i[1] for i in info]
        w = [i[2] for i in info]
        ma = shifted_pair(sext, role[0] * ga[0], role[1] * ga[1])
        m[0:128] = lhs_quad(ma)
        m[128:256] = lhs_quad(ma.T)
        mb = shifted_pair(sext, role[0] * gb[0], role[1] * gb[1])
        m[256:384] = lhs_halves(mb) if lone else lhs_quad(mb)
        m[384:512] = lhs_halves(mb.T) if lone else lhs_quad(mb.T)
        mc = shifted_pair(sext, role[0] * gc[0], role[1] * gc[1])
        m[512:768] = row_quad(mc.T)
        weight = jnp.where(iota((128, 128), 1) < B, w[0], w[1])
        m[768:1024] = row_quad(-mc * weight)
        ii, nn = iota((128, 256), 0), iota((128, 256), 1)
        row, col = iota((B, 256), 0), iota((B, 256), 1)
        for s in range(2):
            hit = ((nn // 64) % 2 == s) & (ii // 64 == nn // 128) & (ii % 64 == nn % 64 + gc[s])
            m[1024 + 128 * s:1152 + 128 * s] = jnp.where(hit, 1.0, 0.0).astype(bf16)
            m[1280 + B * s:1344 + B * s] = jnp.where(col == row + ga[s], 1.0, 0.0).astype(bf16)
            steps[s] = jnp.full((8, 128), gb[s], jnp.int32)


def prepare(tab, calls):
    vm = pl.BlockSpec(memory_space=pltpu.VMEM)
    outs = []
    for _ in calls:
        outs += [OUT((ROWS, 256), bf16), OUT((2, 8, 128), jnp.int32)]
    return pl.pallas_call(
        lambda *refs: prepare_kernel(calls, *refs),
        out_shape=outs, in_specs=[pl.BlockSpec(memory_space=pltpu.SMEM), vm], out_specs=[vm] * len(outs),
        cost_estimate=pl.CostEstimate(flops=3_000_000_000, bytes_accessed=1 << 20, transcendentals=0),
        compiler_params=pltpu.CompilerParams(vmem_limit_bytes=16 << 20),
    )(tab, jnp.asarray(SEXT))


def staggered(count, steps):
    values = {}
    for i in range(count + 2 * (len(steps) - 1)):
        for j, step in enumerate(steps):
            t = i - 2 * j
            if 0 <= t < count:
                values[t] = step(t, values.pop(t, None))


def pair_kernel(TB, TA, first, last, lone, x_hbm, n0_ref, n1_ref, acc_ref, m, steps, lev_ref, la_ref, out_ref,
                x_ref, stage_ref, sems, xp0, xp1, y_ref, z_ref):
    load = pltpu.make_async_copy(x_hbm, x_ref, sems.at[0])
    load.start()
    if first:
        load.wait()
        n0_ref = x_ref
    gb = [jnp.max(steps[s]) for s in range(2)]
    lane = iota((B, 128), 1)
    for s, (n_ref, xp) in enumerate(((n0_ref, xp0), (n1_ref, xp1))[:1 if lone else 2]):
        xp[:, :1024] = jnp.zeros((B, 1024), bf16)
        xp[:, 5120:] = jnp.zeros((B, 1024), bf16)
        odd = gb[s] & 1
        keep = lane < jnp.where(odd == 1, B, 2 * B)
        before = jnp.zeros((B, 128), f32)
        for i in range(4):
            v = dot(m[1280 + B * s:1344 + B * s, :B], n_ref[:, 1024 * i:1024 * i + 1024])
            for j in range(8):
                col = pltpu.roll(v[:, 128 * j:128 * j + 128], 64 * odd, 1)
                at = 1024 * i + 128 * j + 896
                xp[:, at:at + 128] = jnp.where(keep, before, col).astype(bf16)
                before = col
        xp[:, 4992:5120] = jnp.where(keep, before, 0.0).astype(bf16)
    if not first:
        load.wait()
    q0, q1 = 8 + (gb[0] >> 1), 8 + (gb[1] >> 1)
    if lone:
        q1, xp1 = q0 + 16, xp0
    pairs = 16 if lone else 32

    def moved(t, _):
        wins = []
        for j in range(TB):
            bp = t * TB + j
            l0 = pl.multiple_of((bp + q0) * 128, 128)
            l1 = pl.multiple_of((bp + q1) * 128, 128)
            wins.append(jnp.concatenate([xp0[:, pl.ds(l0, 128)], xp1[:, pl.ds(l1, 128)]], 1))
        return dot(jnp.concatenate(wins, 0), m[1024:1280])

    def density(t, y):
        even, odds = [], []
        for j in range(TB):
            bp = t * TB + j
            v = x_ref[:, 128 * bp:128 * bp + 128].astype(f32)
            u = x_ref[:, 128 * bp + 2048:128 * bp + 2176].astype(f32) if lone else v
            r = pltpu.roll(v, 64, 1)
            even.append(jnp.where(lane < B, v, pltpu.roll(u, 64, 1) if lone else r))
            odds.append(jnp.where(lane < B, r, u))
            for o in range(2):
                y_ref[t * 2 * TB + 2 * j + o] = y[64 * j:64 * j + 64, 128 * o:128 * o + 128].astype(bf16)
        d = jnp.concatenate([y[:, :128], y[:, 128:]], 0) * jnp.concatenate(even + odds, 0)
        return rows_through(d, m[512:768])

    def first_forward(t, d):
        d = jnp.concatenate([d[64 * (o * TB + j):64 * (o * TB + j) + 64] for j in range(TB) for o in range(2)], 1)
        d = cols_through(m[0:B if lone else 128], d)
        for k in range(2 * TB):
            at = (t * 2 * TB + k) * PITCH
            z_ref[at:at + 64, :] = d[:, 128 * k:128 * k + 128]

    staggered(pairs // TB, (moved, density, first_forward))

    lev = lev_ref[...]
    if lone:
        lev = jnp.where(iota((32, 128), 1) < B, lev[:32], lev[32:])
    deep = 32 if lone else 64
    through = (lambda a, d: halves_through(m[a:a + 128, :128], d)) if lone else (lambda a, d: cols_through(m[a:a + 128], d))

    def second_forward(t, _):
        parts = [z_ref[pl.ds(t * TA + k, deep, stride=PITCH), :] for k in range(TA)]
        d = through(256, jnp.concatenate(parts, 1))
        g = jnp.concatenate([1.0 / (lev + la_ref[t * TA + k:t * TA + k + 1, :]) for k in range(TA)], 1)
        return d * g

    def second_back(t, d):
        d = through(384, d)
        for k in range(TA):
            z_ref[pl.ds(t * TA + k, deep, stride=PITCH), :] = d[:, 128 * k:128 * k + 128]

    staggered(64 // TA, (second_forward, second_back))

    stores = []
    target = stage_ref if last else out_ref

    def first_back(t, _):
        parts = [z_ref[(t * 2 * TB + k) * PITCH:(t * 2 * TB + k) * PITCH + 64, :] for k in range(2 * TB)]
        return cols_through(m[128:192 if lone else 256], jnp.concatenate(parts, 1))

    def last_back(t, d):
        d = jnp.concatenate([d[:, 128 * k:128 * k + 128] for k in range(2 * TB)], 0)
        d = rows_through(d, m[768:1024])
        for j in range(TB):
            v = [d[64 * k:64 * k + 64] * y_ref[t * 2 * TB + k].astype(f32) for k in (2 * j, 2 * j + 1)]
            at = (t * TB + j) * 128
            if lone:
                low = jnp.where(lane < B, v[0], pltpu.roll(v[1], 64, 1))
                high = jnp.where(lane < B, pltpu.roll(v[0], 64, 1), v[1])
                target[:, at:at + 128] = acc_ref[:, at:at + 128] + low
                target[:, at + 2048:at + 2176] = acc_ref[:, at + 2048:at + 2176] + high
            else:
                r = jnp.where(lane < B, v[0], v[1]) + pltpu.roll(jnp.where(lane < B, v[1], v[0]), 64, 1)
                target[:, at:at + 128] = r if first else acc_ref[:, at:at + 128] + r
        if last:
            for at in (t * TB * 128, t * TB * 128 + 2048)[:2 if lone else 1]:
                part = pl.ds(at, TB * 128)
                stores.append(pltpu.make_async_copy(stage_ref.at[:, part], out_ref.at[:, part], sems.at[1 + len(stores)]))
                stores[-1].start()

    staggered(pairs // TB, (first_back, last_back))
    for store in stores:
        store.wait()


def pair_call(made, x, n0, n1, acc, last=False, TB=4, TA=8, LB=4):
    first, lone = acc is None, n1 is None
    TB = min(TB, LB) if lone else TB
    vm = pl.BlockSpec(memory_space=pltpu.VMEM)
    hbm = pl.BlockSpec(memory_space=pl.ANY)
    args = [x] + ([] if first else [n0]) + ([] if lone else [n1]) + ([] if first else [acc])
    args += [*made, jnp.asarray(LEV), jnp.asarray(LA)]
    specs = [hbm] + [vm] * (len(args) - 1)

    def body(*refs):
        refs = list(refs)
        if first:
            refs.insert(1, None)
        if lone:
            refs.insert(2, refs[1])
        if first:
            refs.insert(3, None)
        pair_kernel(TB, TA, first, last, lone, *refs)

    return pl.pallas_call(
        body,
        out_shape=jax.ShapeDtypeStruct((B, B * B), f32) if last else OUT((B, B * B), f32),
        in_specs=specs, out_specs=hbm if last else vm,
        scratch_shapes=[
            pltpu.VMEM((B, B * B), bf16), pltpu.VMEM((B, B * B) if last else (8, 128), f32),
            pltpu.SemaphoreType.DMA((1 + 32 // TB,)),
            pltpu.VMEM((B, 6144), bf16), pltpu.VMEM((B, 6144), bf16),
            pltpu.VMEM((B, B, 128), bf16), pltpu.VMEM((B * PITCH + 8, 128), f32),
        ],
        cost_estimate=pl.CostEstimate(flops=10_000_000_000, bytes_accessed=4 << 20, transcendentals=0),
        compiler_params=pltpu.CompilerParams(vmem_limit_bytes=32 << 20),
    )(*args)


def permute(value, target):
    count = lax.axis_size(AXES)
    return lax.ppermute(value, AXES, [(p, target(p) % count) for p in range(count)])


def per_device(orbitals, offsets, pair_list):
    x = orbitals.reshape(B, B * B)
    tab = jnp.concatenate([offsets.T, pair_list.T], 0)
    swap = lambda p: p ^ 1
    near = permute(x, lambda p: p + 2 if p % 2 else p - 2)
    own = permute(x, swap)
    made = prepare(tab, ((0, 1), (2, -1), (-2, None), (3, -3)))
    later, mine = lax.optimization_barrier((x, made[0]))
    back = permute(later, lambda p: p - 2 if p % 2 else p + 2)
    acc = pair_call([mine, made[1]], x, x, own, None)
    near, acc = lax.optimization_barrier((near, acc))
    far = permute(near, lambda p: p + 1 if p % 2 else p - 1)
    near_swap = permute(near, swap)
    acc = pair_call(made[2:4], x, near, near_swap, acc)
    back, acc = lax.optimization_barrier((back, acc))
    back_swap = permute(back, swap)
    acc = pair_call(made[4:6], x, back, None, acc)
    acc = pair_call(made[6:8], x, back_swap, far, acc, last=True)
    return acc.reshape(orbitals.shape)


def solution(mesh):
    in_specs = (P(AXES, None, None), P(), P())
    return jax.shard_map(
        per_device, mesh=mesh, in_specs=in_specs, out_specs=P(AXES, None, None), check_vma=False
    )
```
